32 devices in a mesh: dp: 2 (over core), expert: 16 (over z, y, x).
Axes of the slice: x: 2, y: 2, z: 4, core: 2. Of those that a mesh axis runs over, the one named last changes fastest.
Arguments:
- tokens: bfloat16 [8192, 1280], P(('dp', 'expert')), may hold values from -48 to 48
- phi: bfloat16 [1280, 48], replicated, may hold values from -0.05 to 0.05
- slot_count: int32 [16], replicated, may hold values from 1 to 3, 40 in all
- w_in: bfloat16 [16, 2560, 1280], P('expert'), may hold values from -1.25 to 1.25
- w_out: bfloat16 [16, 2560, 1280], P('expert'), may hold values from -1 to 1
- grad_out: bfloat16 [8192, 1280], P(('dp', 'expert')), may hold values from -6 to 6
Outputs:
- mixed_out: bfloat16 [8192, 1280], P(('dp', 'expert'))
- grad_tokens: bfloat16 [8192, 1280], P(('dp', 'expert'))
- grad_phi: float32 [1280, 48], replicated
- grad_w_in: bfloat16 [16, 2560, 1280], P('expert', 'dp')
- grad_w_out: bfloat16 [16, 2560, 1280], P('expert', 'dp')
The draws below stay inside these ranges and needn't reach their ends.
Inputs may be any that keep to these rules, and one draw needn't show every extreme that they name: slot_count sums to 40; some expert has exactly 3.
All inputs are finite; a program needn't handle non-finite values.
Results may differ from the reference program's by a relative error of at most 0.012.
The reference program's roundings to bfloat16 on the way count: a program that leaves them out, or rounds other values in their place, can miss the bound.
Values may be sent and summed in bfloat16 or wider, within the bound.
A program may use at most 128 MiB of HBM per device.

```python
import math
import jax
import jax.numpy as jnp
import numpy as np
from jax import lax

D = 1280
FF = 2560
TOK = 256
MOST = 3
EXPERTS = 16
SLOTS = 40
IMAGES = 32
TOKENS = 8192


def phi_entries(key):
    return jax.random.uniform(jax.random.fold_in(key, 11), (D, EXPERTS * MOST), jnp.float32, minval=-0.0495, maxval=0.0495)


def draw_phi(key, part):
    return phi_entries(key).astype(jnp.bfloat16)


def draw_tokens(key, part):
    samples = jax.random.normal(jax.random.fold_in(key, 23), (IMAGES, TOK, D), jnp.float32)
    return jnp.clip(samples, -48.0, 48.0).reshape(TOKENS, D).astype(jnp.bfloat16)


def block_levels(own_key, shape, cuts, least, high):
    def one(axis_at, blocks):
        draws = jax.random.uniform(jax.random.fold_in(jax.random.fold_in(own_key, 6), axis_at), (blocks,), jnp.float32, least / len(cuts), high / len(cuts))
        return jnp.repeat(jnp.exp(draws), shape[axis_at] // blocks).reshape((-1,) + (1,) * (len(shape) - axis_at - 1))

    level = one(*cuts[0])
    for cut in cuts[1:]:
        level = level * one(*cut)
    return level


def length_profile(amount, total, bound, skew):
    portions = [(1 << 20) // math.isqrt(grade ** skew) + 1 for grade in range(2, amount + 1)]
    rest, given = total - bound - (amount - 1), [1] * (amount - 1)
    while rest > 0:
        candidates = [i for i in range(amount - 1) if given[i] < bound]
        mass, left = sum([portions[i] for i in candidates]), rest
        for i in candidates:
            addition = min(bound - given[i], max(1, left * portions[i] // mass), rest)
            given[i] = given[i] + addition
            rest = rest - addition
    return np.array([bound] + given)


def ragged(rng, number_of, total, most, slope):
    if number_of == 2:
        one = jax.random.randint(rng, (), max(1, total - most), min(most, total - 1) + 1)
        return jnp.stack([one, total - one])
    lengths = jnp.asarray(length_profile(number_of, total, most, slope), jnp.int32)
    pairs = (number_of - 1) // 2
    source_of, sink = lengths[1:1 + 2 * pairs:2], lengths[2:2 + 2 * pairs:2]
    margin = jnp.minimum(source_of - 1, most - sink)
    passed = jax.random.randint(jax.random.fold_in(rng, 1), (pairs,), 0, 1 << 20) % (margin + 1)
    lengths = lengths.at[1:1 + 2 * pairs:2].set(source_of - passed).at[2:2 + 2 * pairs:2].set(sink + passed)
    return lengths[jax.random.permutation(jax.random.fold_in(rng, 2), number_of)]


def noise(rng, shape, scale, most, cuts=(), held_as=jnp.bfloat16):
    loudness = block_levels(rng, shape, cuts, -0.22, 0.18) if cuts else 1.0
    entries = jax.random.normal(rng, shape, jnp.float32) * scale * loudness
    return jnp.minimum(jnp.maximum(entries, -most), most).astype(held_as)


def setup_inputs(seed: int = 0) -> dict:
    key_list = jax.random.split(jax.random.key(seed), 7)
    tokens = draw_tokens(jax.random.fold_in(key_list[6], 71), 0)
    phi = draw_phi(jax.random.fold_in(key_list[6], 71), 0)
    slot_count = ragged(key_list[2], EXPERTS, SLOTS, MOST, 2).astype(jnp.int32)
    w_in = noise(key_list[3], (EXPERTS, FF, D), (max(D // 64, 4)) ** -0.5, 1.25, ((0, 16),))
    w_out = noise(key_list[4], (EXPERTS, FF, D), (max(FF // 64, 4)) ** -0.5, 1.0, ((0, 16),))
    grad_out = noise(key_list[5], (TOKENS, D), 1.0, 6.0, ((0, 32),))
    return {"tokens": tokens, "phi": phi, "slot_count": slot_count, "w_in": w_in, "w_out": w_out, "grad_out": grad_out}


SQRT_HALF = 0.7071067811865476
INV_SQRT_TAU = 0.3989422804014327


def contract(left, right, left_dim, right_dim):
    return lax.dot_general(left, right, (((left_dim,), (right_dim,)), ((), ())), preferred_element_type=jnp.float32)


def softmax_along(logits, axis):
    maximum = jnp.max(logits, axis=axis, keepdims=True)
    weights = jnp.exp(logits - maximum)
    return weights / jnp.sum(weights, axis=axis, keepdims=True)


def gelu_parts(preact):
    normal_cdf = 0.5 * (1.0 + jax.scipy.special.erf(preact * SQRT_HALF))
    density = jnp.exp(-0.5 * preact * preact) * INV_SQRT_TAU
    return preact * normal_cdf, normal_cdf + preact * density


def live_slots(slot_count):
    positions = lax.broadcasted_iota(jnp.int32, (slot_count.shape[0], MOST), 1)
    return (positions < slot_count[:, None]).reshape(-1)


def image_front(image_tokens, phi, live_mask):
    logits = jnp.dot(image_tokens, phi, preferred_element_type=jnp.float32)
    spread = softmax_along(logits, 0)
    spread_b = spread.astype(jnp.bfloat16)
    slot_in = contract(spread_b, image_tokens, 0, 0).astype(jnp.bfloat16)
    mixing = softmax_along(jnp.where(live_mask[None, :], logits, -1e30), 1)
    return slot_in, spread, spread_b, mixing


def image_returned(image_tokens, phi, output_cotangent, slot_values, slot_grads, spread, spread_b, mixing):
    d_mix = contract(output_cotangent, slot_values, 1, 1)
    d_comb = mixing * (d_mix - jnp.sum(d_mix * mixing, axis=1, keepdims=True))
    d_spread = contract(image_tokens, slot_grads, 1, 1)
    d_disp = spread * (d_spread - jnp.sum(d_spread * spread, axis=0, keepdims=True))
    d_logits = (d_comb + d_disp).astype(jnp.bfloat16)
    image_gradient = contract(d_logits, phi, 1, 1) + jnp.dot(spread_b, slot_grads, preferred_element_type=jnp.float32)
    return image_gradient.astype(jnp.bfloat16), contract(image_tokens, d_logits, 0, 0)


def expert_front(slot_rows, first_proj, second_proj):
    preact = contract(slot_rows, first_proj, 1, 1)
    activated, slopes = gelu_parts(preact)
    hidden = activated.astype(jnp.bfloat16)
    return jnp.dot(hidden, second_proj, preferred_element_type=jnp.float32), hidden, slopes


def expert_back(slot_rows, hidden, slopes, row_grads, first_proj, second_proj):
    d_hidden = contract(row_grads, second_proj, 1, 1)
    grad_pre = (d_hidden * slopes).astype(jnp.bfloat16)
    grad_rows = jnp.dot(grad_pre, first_proj, preferred_element_type=jnp.float32)
    grad_first = contract(grad_pre, slot_rows, 0, 0)
    grad_second = contract(hidden, row_grads, 0, 0)
    return grad_rows, grad_first, grad_second


def to_experts(array):
    return array.reshape(IMAGES, EXPERTS, MOST, D).transpose(1, 0, 2, 3).reshape(EXPERTS, IMAGES * MOST, D)


def to_images(array):
    return array.reshape(EXPERTS, IMAGES, MOST, D).transpose(1, 0, 2, 3).reshape(IMAGES, EXPERTS * MOST, D)


def reference(tokens, phi, slot_count, w_in, w_out, grad_out):
    live_mask = live_slots(slot_count)
    images = tokens.reshape(IMAGES, TOK, D)
    cotangents = grad_out.reshape(IMAGES, TOK, D)

    def front(packed_group):
        image_tokens, output_cotangent = packed_group
        slot_in, spread, spread_b, mixing = image_front(image_tokens, phi, live_mask)
        mixing_b = mixing.astype(jnp.bfloat16)
        slot_cot = contract(mixing_b, output_cotangent, 0, 0).astype(jnp.bfloat16)
        return slot_in, slot_cot, spread, spread_b, mixing, mixing_b

    slot_in, slot_cot, spread, spread_b, mixing, mixing_b = lax.map(front, (images, cotangents))

    def expert(packed_group):
        slot_rows, row_grads, first_proj, second_proj = packed_group
        values, hidden, slopes = expert_front(slot_rows, first_proj, second_proj)
        grad_rows, grad_first, grad_second = expert_back(slot_rows, hidden, slopes, row_grads, first_proj, second_proj)
        return (values.astype(jnp.bfloat16), grad_rows.astype(jnp.bfloat16),
                grad_first.astype(jnp.bfloat16), grad_second.astype(jnp.bfloat16))

    values, grad_rows, grad_w_in, grad_w_out = lax.map(expert, (to_experts(slot_in), to_experts(slot_cot), w_in, w_out))
    slot_values = to_images(values)
    slot_grads = to_images(grad_rows)

    def back(packed_group):
        image_tokens, output_cotangent, slot_state, slot_gradient, dispatch_weight, dispatch_weight_batch, combine_weight, combine_weight_batch = packed_group
        combined_output = jnp.dot(combine_weight_batch, slot_state, preferred_element_type=jnp.float32).astype(jnp.bfloat16)
        image_gradient, gradient_piece = image_returned(image_tokens, phi, output_cotangent, slot_state, slot_gradient, dispatch_weight, dispatch_weight_batch, combine_weight)
        return combined_output, image_gradient, gradient_piece

    combined_output, grad_images, grad_terms = lax.map(back, (images, cotangents, slot_values, slot_grads, spread, spread_b, mixing, mixing_b))
    grad_phi = jnp.sum(grad_terms, axis=0)
    return combined_output.reshape(TOKENS, D), grad_images.reshape(TOKENS, D), grad_phi, grad_w_in, grad_w_out
```

```python
import jax
import jax.numpy as jnp
from jax import lax
from jax.sharding import PartitionSpec as P

D = 1280
MOST = 3


SQRT_HALF = 0.7071067811865476
INV_SQRT_TAU = 0.3989422804014327


def contract(left, right, left_dim, right_dim):
    return lax.dot_general(
        left, right, (((left_dim,), (right_dim,)), ((), ())), preferred_element_type=jnp.float32
    )


def softmax_along(logits, axis):
    maximum = jnp.max(logits, axis=axis, keepdims=True)
    weights = jnp.exp(logits - maximum)
    return weights / jnp.sum(weights, axis=axis, keepdims=True)


def gelu_parts(preact):
    normal_cdf = 0.5 * (1.0 + jax.scipy.special.erf(preact * SQRT_HALF))
    density = jnp.exp(-0.5 * preact * preact) * INV_SQRT_TAU
    return (preact * normal_cdf, normal_cdf + preact * density)


def live_slots(slot_count):
    positions = lax.broadcasted_iota(jnp.int32, (slot_count.shape[0], MOST), 1)
    return (positions < slot_count[:, None]).reshape(-1)


def image_front(image_tokens, phi, live_mask):
    logits = jnp.dot(image_tokens, phi, preferred_element_type=jnp.float32)
    spread = softmax_along(logits, 0)
    spread_b = spread.astype(jnp.bfloat16)
    slot_in = contract(spread_b, image_tokens, 0, 0).astype(jnp.bfloat16)
    mixing = softmax_along(jnp.where(live_mask[None, :], logits, -1e30), 1)
    return (slot_in, spread, spread_b, mixing)


def image_returned(
    image_tokens, phi, output_cotangent, slot_values, slot_grads, spread, spread_b, mixing
):
    d_mix = contract(output_cotangent, slot_values, 1, 1)
    d_comb = mixing * (d_mix - jnp.sum(d_mix * mixing, axis=1, keepdims=True))
    d_spread = contract(image_tokens, slot_grads, 1, 1)
    d_disp = spread * (d_spread - jnp.sum(d_spread * spread, axis=0, keepdims=True))
    d_logits = (d_comb + d_disp).astype(jnp.bfloat16)
    image_gradient = contract(d_logits, phi, 1, 1) + jnp.dot(
        spread_b, slot_grads, preferred_element_type=jnp.float32
    )
    return (image_gradient.astype(jnp.bfloat16), contract(d_logits, image_tokens, 0, 0))


def expert_front(slot_rows, first_proj, second_proj):
    preact = contract(slot_rows, first_proj, 1, 1)
    activated, slopes = gelu_parts(preact)
    hidden = activated.astype(jnp.bfloat16)
    return (jnp.dot(hidden, second_proj, preferred_element_type=jnp.float32), hidden, slopes)


def expert_back(slot_rows, hidden, slopes, row_grads, first_proj, second_proj):
    d_hidden = contract(row_grads, second_proj, 1, 1)
    grad_pre = (d_hidden * slopes).astype(jnp.bfloat16)
    grad_rows = jnp.dot(grad_pre, first_proj, preferred_element_type=jnp.float32)
    grad_first = contract(grad_pre, slot_rows, 0, 0)
    grad_second = contract(hidden, row_grads, 0, 0)
    return (grad_rows, grad_first, grad_second)


def sum_own_half(partial):
    rows = partial.shape[0] // 2
    mine = lax.axis_index("dp")
    kept = lax.dynamic_slice_in_dim(partial, mine * rows, rows, 0)
    given = lax.dynamic_slice_in_dim(partial, (1 - mine) * rows, rows, 0)
    return kept + lax.ppermute(given, "dp", [(0, 1), (1, 0)])


def sum_everywhere(term, experts):
    swap = [(0, 1), (1, 0)]
    half = D // 2
    mine = lax.axis_index("dp")
    kept = lax.dynamic_slice_in_dim(term, mine * half, half, 1)
    given = lax.dynamic_slice_in_dim(term, (1 - mine) * half, half, 1)
    term = kept + lax.ppermute(given, "dp", swap)
    pieces = lax.all_to_all(
        term.reshape(experts, -1, 128), "expert", split_axis=0, concat_axis=0, tiled=True
    )
    piece = jnp.sum(pieces, axis=0)
    copies = jnp.broadcast_to(piece[None], (experts,) + piece.shape)
    whole = lax.all_to_all(copies, "expert", split_axis=0, concat_axis=0, tiled=True)
    whole = whole.reshape(-1, half)
    other = lax.ppermute(whole, "dp", swap)
    first = jnp.where(mine == 0, whole, other)
    second = jnp.where(mine == 0, other, whole)
    return jnp.concatenate([first, second], axis=1).T


def local(tokens, phi, slot_count, w_in, w_out, grad_out):
    live_mask = live_slots(slot_count)
    experts = slot_count.shape[0]
    slot_in, spread, spread_b, mixing = image_front(tokens, phi, live_mask)
    mixing_b = mixing.astype(jnp.bfloat16)
    slot_cot = contract(mixing_b, grad_out, 0, 0).astype(jnp.bfloat16)
    outgoing = jnp.concatenate([slot_in, slot_cot], axis=1).reshape(experts, -1, 128)
    arrived = lax.all_to_all(outgoing, "expert", split_axis=0, concat_axis=0, tiled=True)
    arrived = arrived.reshape(-1, 2 * D)
    first_proj = w_in[0]
    second_proj = w_out[0]
    half_width = first_proj.shape[0] // lax.axis_size("dp")
    offset = lax.axis_index("dp") * half_width
    first_half = lax.dynamic_slice_in_dim(first_proj, offset, half_width, 0)
    second_half = lax.dynamic_slice_in_dim(second_proj, offset, half_width, 0)
    both = lax.all_gather(arrived, "dp", axis=0, tiled=True)
    both_rows, both_grads = both[:, :D], both[:, D:]
    values, hidden, slopes = expert_front(both_rows, first_half, second_half)
    grad_rows, grad_first, grad_second = expert_back(
        both_rows, hidden, slopes, both_grads, first_half, second_half
    )
    values = sum_own_half(values)
    grad_rows = sum_own_half(grad_rows)
    returning = jnp.concatenate(
        [values.astype(jnp.bfloat16), grad_rows.astype(jnp.bfloat16)], axis=1
    ).reshape(lax.axis_size("expert"), -1, 128)
    back = lax.all_to_all(returning, "expert", split_axis=0, concat_axis=0, tiled=True)
    back = back.reshape(-1, 2 * D)
    slot_values, slot_grads = back[:, :D], back[:, D:]
    mixed_out = jnp.dot(mixing_b, slot_values, preferred_element_type=jnp.float32).astype(
        jnp.bfloat16
    )
    grad_tokens, gradient_piece = image_returned(
        tokens, phi, grad_out, slot_values, slot_grads, spread, spread_b, mixing
    )
    grad_phi = sum_everywhere(gradient_piece, experts)
    return (
        mixed_out,
        grad_tokens,
        grad_phi,
        grad_first.astype(jnp.bfloat16)[None],
        grad_second.astype(jnp.bfloat16)[None],
    )


def solution(mesh):
    placed = (
        P(("dp", "expert"), None),
        P(),
        P(),
        P("expert", None, None),
        P("expert", None, None),
        P(("dp", "expert"), None),
    )

    return jax.shard_map(
        local,
        mesh=mesh,
        in_specs=placed,
        out_specs=(
            P(("dp", "expert"), None),
            P(("dp", "expert"), None),
            P(),
            P("expert", "dp", None),
            P("expert", "dp", None),
        ),
        check_vma=False,
    )
```

```python
import jax
import jax.numpy as jnp
from jax import lax
from jax.sharding import PartitionSpec as P

D = 1280
MOST = 3


SQRT_HALF = 0.7071067811865476
INV_SQRT_TAU = 0.3989422804014327


def contract(left, right, left_dim, right_dim):
    return lax.dot_general(
        left, right, (((left_dim,), (right_dim,)), ((), ())), preferred_element_type=jnp.float32
    )


def softmax_along(logits, axis):
    maximum = jnp.max(logits, axis=axis, keepdims=True)
    weights = jnp.exp(logits - maximum)
    return weights / jnp.sum(weights, axis=axis, keepdims=True)


def gelu_parts(preact):
    normal_cdf = 0.5 * (1.0 + jax.scipy.special.erf(preact * SQRT_HALF))
    density = jnp.exp(-0.5 * preact * preact) * INV_SQRT_TAU
    return (preact * normal_cdf, normal_cdf + preact * density)


def live_slots(slot_count):
    positions = lax.broadcasted_iota(jnp.int32, (slot_count.shape[0], MOST), 1)
    return (positions < slot_count[:, None]).reshape(-1)


def image_front(image_tokens, phi, live_mask):
    logits = jnp.dot(image_tokens, phi, preferred_element_type=jnp.float32)
    spread = softmax_along(logits, 0)
    spread_b = spread.astype(jnp.bfloat16)
    slot_in = contract(spread_b, image_tokens, 0, 0).astype(jnp.bfloat16)
    mixing = softmax_along(jnp.where(live_mask[None, :], logits, -1e30), 1)
    return (slot_in, spread, spread_b, mixing)


def image_returned(
    image_tokens, phi, output_cotangent, slot_values, slot_grads, spread, spread_b, mixing
):
    d_mix = contract(output_cotangent, slot_values, 1, 1)
    d_comb = mixing * (d_mix - jnp.sum(d_mix * mixing, axis=1, keepdims=True))
    d_spread = contract(image_tokens, slot_grads, 1, 1)
    d_disp = spread * (d_spread - jnp.sum(d_spread * spread, axis=0, keepdims=True))
    d_logits = (d_comb + d_disp).astype(jnp.bfloat16)
    image_gradient = contract(d_logits, phi, 1, 1) + jnp.dot(
        spread_b, slot_grads, preferred_element_type=jnp.float32
    )
    return (image_gradient.astype(jnp.bfloat16), contract(d_logits, image_tokens, 0, 0))


def expert_front(slot_rows, first_proj, second_proj):
    preact = contract(slot_rows, first_proj, 1, 1)
    activated, slopes = gelu_parts(preact)
    hidden = activated.astype(jnp.bfloat16)
    return (jnp.dot(hidden, second_proj, preferred_element_type=jnp.float32), hidden, slopes)


def expert_back(slot_rows, hidden, slopes, row_grads, first_proj, second_proj):
    d_hidden = contract(row_grads, second_proj, 1, 1)
    grad_pre = (d_hidden * slopes).astype(jnp.bfloat16)
    grad_rows = jnp.dot(grad_pre, first_proj, preferred_element_type=jnp.float32)
    grad_first = contract(grad_pre, slot_rows, 0, 0)
    grad_second = contract(hidden, row_grads, 0, 0)
    return (grad_rows, grad_first, grad_second)


def sum_own_half(partial):
    rows = partial.shape[0] // 2
    kept, given = partial[:rows], partial[rows:]
    return kept + lax.ppermute(given, "dp", [(0, 1), (1, 0)])


def sum_everywhere(term, experts):
    swap = [(0, 1), (1, 0)]
    half = D // 2
    mine = lax.axis_index("dp")
    kept = lax.dynamic_slice_in_dim(term, mine * half, half, 1)
    given = lax.dynamic_slice_in_dim(term, (1 - mine) * half, half, 1)
    term = kept + lax.ppermute(given, "dp", swap)
    pieces = lax.all_to_all(
        term.reshape(experts, -1, 128), "expert", split_axis=0, concat_axis=0, tiled=True
    )
    piece = jnp.sum(pieces, axis=0)
    copies = jnp.broadcast_to(piece[None], (experts,) + piece.shape)
    whole = lax.all_to_all(copies, "expert", split_axis=0, concat_axis=0, tiled=True)
    whole = whole.reshape(-1, half)
    other = lax.ppermute(whole, "dp", swap)
    first = jnp.where(mine == 0, whole, other)
    second = jnp.where(mine == 0, other, whole)
    return jnp.concatenate([first, second], axis=1).T


def local(tokens, phi, slot_count, w_in, w_out, grad_out):
    live_mask = live_slots(slot_count)
    experts = slot_count.shape[0]
    slot_in, spread, spread_b, mixing = image_front(tokens, phi, live_mask)
    mixing_b = mixing.astype(jnp.bfloat16)
    slot_cot = contract(mixing_b, grad_out, 0, 0).astype(jnp.bfloat16)
    outgoing = jnp.concatenate([slot_in, slot_cot], axis=1).reshape(experts, -1, 128)
    arrived = lax.all_to_all(outgoing, "expert", split_axis=0, concat_axis=0, tiled=True)
    arrived = arrived.reshape(-1, 2 * D)
    first_proj = w_in[0]
    second_proj = w_out[0]
    half_width = first_proj.shape[0] // lax.axis_size("dp")
    offset = lax.axis_index("dp") * half_width
    first_half = lax.dynamic_slice_in_dim(first_proj, offset, half_width, 0)
    second_half = lax.dynamic_slice_in_dim(second_proj, offset, half_width, 0)
    both = jnp.concatenate([arrived, lax.ppermute(arrived, "dp", [(0, 1), (1, 0)])], axis=0)
    both_rows, both_grads = both[:, :D], both[:, D:]
    values, hidden, slopes = expert_front(both_rows, first_half, second_half)
    grad_rows, grad_first, grad_second = expert_back(
        both_rows, hidden, slopes, both_grads, first_half, second_half
    )
    values = sum_own_half(values)
    grad_rows = sum_own_half(grad_rows)
    returning = jnp.concatenate(
        [values.astype(jnp.bfloat16), grad_rows.astype(jnp.bfloat16)], axis=1
    ).reshape(lax.axis_size("expert"), -1, 128)
    back = lax.all_to_all(returning, "expert", split_axis=0, concat_axis=0, tiled=True)
    back = back.reshape(-1, 2 * D)
    slot_values, slot_grads = back[:, :D], back[:, D:]
    mixed_out = jnp.dot(mixing_b, slot_values, preferred_element_type=jnp.float32).astype(
        jnp.bfloat16
    )
    grad_tokens, gradient_piece = image_returned(
        tokens, phi, grad_out, slot_values, slot_grads, spread, spread_b, mixing
    )
    grad_phi = sum_everywhere(gradient_piece, experts)
    return (
        mixed_out,
        grad_tokens,
        grad_phi,
        grad_first.astype(jnp.bfloat16)[None],
        grad_second.astype(jnp.bfloat16)[None],
    )


def solution(mesh):
    placed = (
        P(("dp", "expert"), None),
        P(),
        P(),
        P("expert", None, None),
        P("expert", None, None),
        P(("dp", "expert"), None),
    )

    return jax.shard_map(
        local,
        mesh=mesh,
        in_specs=placed,
        out_specs=(
            P(("dp", "expert"), None),
            P(("dp", "expert"), None),
            P(),
            P("expert", "dp", None),
            P("expert", "dp", None),
        ),
        check_vma=False,
    )
```
